32 devices in a mesh: node: 8 (over z, core), expert: 4 (over y, x).
Axes of the slice: x: 2, y: 2, z: 4, core: 2. Of those that a mesh axis runs over, the one named last changes fastest.
Arguments:
- numerators: bfloat16 [8, 4, 1536, 1536], P('node', 'expert'), may hold values from -6 to 6
- push_weights: float32 [8], replicated, may hold values from 0.5 to 2
- tokens: bfloat16 [8, 512, 1536], P('node', 'expert'), may hold values from -6 to 6
- cotangent: bfloat16 [8, 512, 1536], P('node', 'expert'), may hold values from -6 to 6
- routing: int32 [8, 512, 2], P('node', 'expert'), may hold values from 0 to 3, all different within a row; in each aligned block of 128 rows (0 to 127, 128 to 255, ..., all dimensions but the last counted through in order) at most 81 rows name the same one
- gates: float32 [8, 512, 2], P('node', 'expert'), may hold values from 0.1 to 1
Outputs:
- averaged: float32 [4, 1536, 1536], P('expert', 'node')
The draws below stay inside these ranges and needn't reach their ends.
Inputs may be any that keep to these rules, and one draw needn't show every extreme that they name: `routing`: each row names 2 different experts; in each aligned block of 128 rows (the rows of one device) no expert is named by more than 81 rows, and in some block some expert is named by exactly 81 rows.
All inputs are finite; a program needn't handle non-finite values.
Results may differ from the reference program's by a relative error of at most 0.007.
The reference program's roundings to bfloat16 on the way count: a program that leaves them out, or rounds other values in their place, can miss the bound.
Values may be sent and summed in bfloat16 or wider, within the bound.
A program may use at most 64 MiB of HBM per device.

```python
import math
import jax
import jax.numpy as jnp
import numpy as np
from jax import lax

D = 1536
HID = 512
TOP = 2
ROUNDS = 2
TOK_DEV = 128
EXPERTS = 4
NODES = 8
TOK_NODE = 512
CAP = 81
N_EXPERT = 4


def strengthened(values, rng, source, target, parts, factor):
    owner, partner = [(jnp.arange(values.shape[axis_at]) // (values.shape[axis_at] // parts)).reshape([-1 if axis == axis_at else 1 for axis in range(values.ndim)]) for axis_at in (source, target)]
    chosen = jax.random.permutation(rng, parts)[partner]
    strong = (owner == chosen) | (owner == (partner + parts // 2) % parts)
    return jnp.where(strong, factor * values, values)


def shard_levels(rng, shape, shards, least, high):
    gain = 1.0
    for axis_at, shards_of in shards:
        steps = jax.random.uniform(jax.random.fold_in(jax.random.fold_in(rng, 6), axis_at), (shards_of,), jnp.float32, least / len(shards), high / len(shards))
        gain = gain * jnp.repeat(jnp.exp(steps), shape[axis_at] // shards_of).reshape((-1,) + (1,) * (len(shape) - 1 - axis_at))
    return gain


def assign_block(key, own, number, rows, number_of, top, bound, lean):
    ranking = jax.random.permutation(key, number_of)
    crowded, ordinary = portions_of(number_of, rows * top, bound, lean, True), portions_of(number_of, rows * top, bound, lean, False)
    places = jnp.arange(number_of)

    def named(lengths, rotation):
        used = int((lengths > 0).sum())
        fixed = max(1, used // 4)
        moved = fixed + (places - fixed + rotation * (used - fixed)) % max(1, number_of - fixed)
        return jnp.zeros((number_of,), jnp.int32).at[ranking[jnp.where(places < fixed, places, moved)]].set(jnp.asarray(lengths, jnp.int32))

    lengths = jnp.where(number % 4 == 0, named(crowded, number // 4), named(ordinary, number - number // 4 - 1))
    mixed = jax.random.permutation(jax.random.fold_in(own, 3), number_of)
    donor, taker = mixed[0:number_of // 2 * 2:2], mixed[1:number_of // 2 * 2:2]
    room = jnp.minimum(lengths[donor] - 1, bound - lengths[taker]) // 2
    room = jnp.where((donor == ranking[0]) | (taker == ranking[0]) | (lengths[taker] == 0), 0, jnp.maximum(room, 0))
    moved = jax.random.randint(jax.random.fold_in(own, 4), (number_of // 2,), 0, 1 << 20) % (room + 1)
    lengths = lengths.at[donor].add(-moved).at[taker].add(moved)
    items = jnp.searchsorted(jnp.cumsum(lengths), jnp.arange(rows * top), side="right").astype(jnp.int32)
    table = items.reshape(top, rows).T
    table = table[jax.random.permutation(jax.random.fold_in(own, 1), rows)]
    rotation = jax.random.randint(jax.random.fold_in(own, 2), (rows, 1), 0, top)
    return jnp.take_along_axis(table, (jnp.arange(top)[None, :] + rotation) % top, axis=1)


def portions_of(number_of, total, bound, lean, full):
    weights = [(1 << 20) // math.isqrt(grade ** lean) + 1 for grade in range(1, number_of + 1)]
    largest = bound if full else min(bound, max(-(-total // number_of), total * weights[0] // sum(weights)))
    least = 1 if total - largest >= number_of - 1 else 0
    given, rest = [largest] + [least] * (number_of - 1), total - largest - least * (number_of - 1)
    while rest > 0:
        free = [i for i in range(1, number_of) if given[i] < largest] or [i for i in range(1, number_of) if given[i] < bound]
        mass, remaining = sum([weights[i] for i in free]), rest
        for i in free:
            extra = min(bound - given[i], max(1, remaining * weights[i] // mass), rest)
            given[i] = given[i] + extra
            rest = rest - extra
    return np.array(given)


def bell_draw(stream_key, shape, spread, bound, split=(), dtype=jnp.bfloat16):
    values = jax.random.normal(stream_key, shape, jnp.float32) * spread
    if len(split) > 0:
        values = shard_levels(stream_key, shape, split, -0.22, 0.18) * values
    return jnp.clip(values, min=-bound, max=bound).astype(dtype)


def bell_draw_with(key, extent, deviation, reach, split, heavy, dtype=jnp.bfloat16):
    array = deviation * jax.random.normal(key, extent, jnp.float32)
    if split:
        array = array * shard_levels(key, extent, split, -0.22, 0.18)
    return jnp.clip(strengthened(array, jax.random.fold_in(key, 3), *heavy), -reach, reach).astype(dtype)


def setup_inputs(seed: int = 0) -> dict:
    keys = jax.random.split(jax.random.key(seed), 7)
    numerators = bell_draw_with(keys[0], (NODES, EXPERTS, D, 3 * HID), 1.0, 6.0, ((0, 8), (1, 4)), (0, 2, 8, 2.0))
    push_weights = jnp.clip(jnp.exp(jax.random.uniform(keys[1], (NODES,), jnp.float32, math.log(0.5), math.log(2.0))), 0.5, 2.0)
    tokens = bell_draw(keys[2], (NODES, TOK_NODE, D), 1.0, 6.0, ((0, 8), (1, 4)))
    cotangent = bell_draw(keys[3], (NODES, TOK_NODE, D), 1.0, 6.0, ((0, 8), (1, 4)))
    routing_keys = jax.random.split(jax.random.fold_in(keys[4], 1), NODES * TOK_NODE // TOK_DEV)
    routing_turns = jax.random.permutation(jax.random.fold_in(keys[4], 3), NODES * TOK_NODE // TOK_DEV)
    routing = jax.vmap(lambda own, number: assign_block(jax.random.fold_in(keys[4], 2), own, number, TOK_DEV, EXPERTS, TOP, CAP, 1))(routing_keys, routing_turns).reshape((NODES, TOK_NODE, TOP))
    gates = jnp.clip(jnp.exp(math.log(1.0) - 2.3025851 * jax.random.uniform(keys[5], (NODES, TOK_NODE, TOP), jnp.float32) ** shard_levels(keys[5], (NODES, TOK_NODE, TOP), ((0, 8), (1, 4)), -0.2, 0.2)), 0.1, 1.0)
    return dict(numerators=numerators, push_weights=push_weights, tokens=tokens, cotangent=cotangent, routing=routing, gates=gates)


step_size = 1.0

def expert_update(weights, buffer_inputs, buffer_gradients):
    hidden_units = weights.shape[1] // 3
    model_scale = 1.0 / math.sqrt(weights.shape[0])
    hidden_scale = 1.0 / math.sqrt(hidden_units)
    gate_weight_matrix = weights[:, :hidden_units]
    upward_weight = weights[:, hidden_units:2 * hidden_units]
    downward_weight = weights[:, 2 * hidden_units:]
    gate_pre = jnp.dot(buffer_inputs, gate_weight_matrix, preferred_element_type=jnp.float32) * model_scale
    upper_pre = jnp.dot(buffer_inputs, upward_weight, preferred_element_type=jnp.float32) * model_scale
    sigmoid_gate = jax.nn.sigmoid(gate_pre)
    gated_hidden = (gate_pre * sigmoid_gate * upper_pre).astype(jnp.bfloat16)
    grad_down = jnp.dot(buffer_gradients.T, gated_hidden, preferred_element_type=jnp.float32) * hidden_scale
    grad_act = jnp.dot(buffer_gradients, downward_weight, preferred_element_type=jnp.float32) * hidden_scale
    gate_gradient = (grad_act * upper_pre * sigmoid_gate * (1.0 + gate_pre * (1.0 - sigmoid_gate))).astype(jnp.bfloat16)
    upward_gradient = (grad_act * gate_pre * sigmoid_gate).astype(jnp.bfloat16)
    grad_wgate = jnp.dot(buffer_inputs.T, gate_gradient, preferred_element_type=jnp.float32) * model_scale
    grad_wupper = jnp.dot(buffer_inputs.T, upward_gradient, preferred_element_type=jnp.float32) * model_scale
    return jnp.concatenate([grad_wgate, grad_wupper, grad_down], axis=1)

def node_step(current, weight, node_tokens, node_cot, node_routes, node_gates):
    params = (current.astype(jnp.float32) / weight).astype(jnp.bfloat16)
    slot_rows = CAP * N_EXPERT
    updates = []
    for expert in range(EXPERTS):
        chosen = node_routes == expert
        present = jnp.any(chosen, axis=1)
        gate_sum = lax.optimization_barrier(jnp.sum(jnp.where(chosen, node_gates, 0.0), axis=1))
        ordering = jnp.argsort(jnp.where(present, 0, 1).astype(jnp.int32), stable=True)[:slot_rows]
        occupied = present[ordering]
        buffer_inputs = jnp.where(occupied[:, None], node_tokens[ordering], 0.0).astype(jnp.bfloat16)
        scaled = gate_sum[ordering][:, None] * node_cot[ordering].astype(jnp.float32)
        buffer_gradients = jnp.where(occupied[:, None], scaled, 0.0).astype(jnp.bfloat16)
        gradients = expert_update(params[expert], buffer_inputs, buffer_gradients)
        updates.append((current[expert].astype(jnp.float32) - step_size * gradients).astype(jnp.bfloat16))
    return jnp.stack(updates)

def reference(numerators, push_weights, tokens, cotangent, routing, gates):
    current = numerators
    weights_now = push_weights
    result = jnp.zeros(numerators.shape[1:], jnp.float32)
    for round_index in range(ROUNDS):
        offset = 2 ** round_index

        def one_node(packed):
            return node_step(packed[0], packed[1], packed[2], packed[3], packed[4], packed[5])
        pushed = lax.map(one_node, (current, weights_now, tokens, cotangent, routing, gates))
        mixed_weights = (weights_now + jnp.roll(weights_now, offset)) / 2.0
        rolled = jnp.roll(pushed, offset, axis=0)
        if round_index < ROUNDS - 1:
            current = ((pushed.astype(jnp.float32) + rolled.astype(jnp.float32)) / 2.0).astype(jnp.bfloat16)
            weights_now = mixed_weights
        else:

            def accumulate(carry, packed):
                first, second, weight = packed
                mixed = (first.astype(jnp.float32) + second.astype(jnp.float32)) / 2.0
                return (carry + mixed / weight / NODES, None)
            result, unused = lax.scan(accumulate, result, (pushed, rolled, mixed_weights))
    return result
```

```python
import functools
import math

import jax
import jax.numpy as jnp
from jax import lax
from jax.experimental import pallas as pl
from jax.experimental.pallas import tpu as pltpu
from jax.sharding import PartitionSpec as P

step_size = 1.0


def slots_of(tokens, top, experts):
    cap = 5 * tokens * top // (4 * experts) + 1
    return -(-cap // 16) * 16


def steps_kernel(
    count, experts, cuts, slots,
    pw, z_hbm, x_hbm, g_hbm, routing, gates, out_ref,
    xb, gb, xs, xin, xn, xt, zc, par, hid, rs, rr, second, came, sent, got,
    load_sem, cut_sem, tok_send, tok_recv, fwd_send, fwd_recv, r_send, r_recv,
    pair_send, pair_recv, line_send, line_recv,
):
    bf16, f32 = jnp.bfloat16, jnp.float32
    node, mine = lax.axis_index("node"), lax.axis_index("expert")
    chips = count // 2
    chip, core = node // 2, node % 2
    other = chip * 2 + (1 - core)
    after, before = (node + 1) % count, (node + count - 1) % count
    depth, width = zc.shape[1:]
    part = width // 3
    hidden = part * cuts
    rows = depth // count
    own = x_hbm.shape[0]
    total = experts * slots
    model_scale = 1.0 / math.sqrt(depth)
    hidden_scale = 1.0 / math.sqrt(hidden)
    tile_d = math.gcd(depth, 256)
    MESH = pl.DeviceIdType.MESH

    loads = [
        pltpu.make_async_copy(x_hbm, xb, load_sem.at[0]),
        pltpu.make_async_copy(g_hbm, gb, load_sem.at[1]),
    ]
    for copy in loads:
        copy.start()

    def cut_load(k, j):
        return pltpu.make_async_copy(
            z_hbm.at[:, pl.ds(j * hidden + k * part, part)],
            zc.at[k, :, pl.ds(j * part, part)],
            cut_sem.at[k, j],
        )

    for k in range(cuts):
        for j in range(3):
            cut_load(k, j).start()

    barrier = pltpu.get_barrier_semaphore()
    for d in range(1, experts):
        pl.semaphore_signal(
            barrier, inc=1, device_id={"expert": mine ^ d}, device_id_type=MESH
        )
    for by in (1, count - 1, 2, count - 2):
        pl.semaphore_signal(
            barrier, inc=1, device_id={"node": (node + by) % count}, device_id_type=MESH
        )

    def weight_at(by):
        return pw[(node + by + count) % count]

    def last_at(by):
        total_w = weight_at(by) + weight_at(by - 1) + weight_at(by - 2) + weight_at(by - 3)
        return jnp.full((1, width), total_w * 0.25, f32)

    def factor_at(by):
        return (0.5 / last_at(by) + 0.5 / last_at(by + 2)) / count

    factor = factor_at(0)
    keep = 0.5 * (factor + factor_at(1))
    later = 1.0 / jnp.full((1, width), weight_at(0) + weight_at(-1), f32)

    lanes = lax.broadcasted_iota(jnp.int32, (own, 128), 1)
    first, second_of = routing[:, 0:1] == lanes, routing[:, 1:2] == lanes
    chosen = jnp.where(first, 1.0, jnp.where(second_of, 1.0, 0.0))
    weighed = jnp.where(first, gates[:, 0:1], jnp.where(second_of, gates[:, 1:2], 0.0))
    chosen_t, weighed_t = chosen.T, weighed.T
    ahead = jnp.where(
        lax.broadcasted_iota(jnp.int32, (own, own), 0)
        < lax.broadcasted_iota(jnp.int32, (own, own), 1),
        1.0, 0.0,
    ).astype(bf16)
    place = jnp.dot(chosen_t.astype(bf16), ahead, preferred_element_type=f32)
    place = jnp.where(chosen_t > 0.0, place, -1.0)
    slot = lax.broadcasted_iota(jnp.int32, (slots, own), 0).astype(f32)
    picks = [jnp.where(slot == place[e : e + 1, :], 1.0, 0.0) for e in range(experts)]
    pick = jnp.concatenate(picks, axis=0).astype(bf16)
    row_gates = jnp.concatenate(
        [jnp.sum(p * weighed_t[e : e + 1, :], axis=1, keepdims=True) for e, p in enumerate(picks)],
        axis=0,
    )

    for copy in loads:
        copy.wait()
    wide = math.gcd(depth, 256)
    for i in range(depth // wide):
        at = slice(i * wide, (i + 1) * wide)
        moved_x = jnp.dot(pick, xb[:, at], preferred_element_type=f32).astype(bf16)
        moved_g = (
            row_gates * jnp.dot(pick, gb[:, at], preferred_element_type=f32)
        ).astype(bf16)
        for e in range(experts):
            of = slice(e * slots, (e + 1) * slots)
            xs[e, :, at] = moved_x[of]
            xs[e, :, depth + i * wide : depth + (i + 1) * wide] = moved_g[of]

    pl.semaphore_wait(barrier, experts - 1 + 4)

    def block(d):
        return pl.ds(d * slots, slots)

    def give(d):
        return pltpu.make_async_remote_copy(
            src_ref=xs.at[mine ^ d], dst_ref=xin.at[block(d)],
            send_sem=tok_send.at[d], recv_sem=tok_recv.at[d],
            device_id={"expert": mine ^ d}, device_id_type=MESH,
        )

    def onward(d):
        return pltpu.make_async_remote_copy(
            src_ref=xs.at[mine] if d == 0 else xin.at[block(d)], dst_ref=xn.at[block(d)],
            send_sem=fwd_send.at[d], recv_sem=fwd_recv.at[d],
            device_id={"node": before}, device_id_type=MESH,
        )

    def result(k):
        return pltpu.make_async_remote_copy(
            src_ref=rs.at[k], dst_ref=rr.at[k],
            send_sem=r_send.at[k], recv_sem=r_recv.at[k],
            device_id={"node": after}, device_id_type=MESH,
        )

    def pair(k):
        return pltpu.make_async_remote_copy(
            src_ref=second.at[k, :, 1 - core], dst_ref=came.at[k],
            send_sem=pair_send.at[k], recv_sem=pair_recv.at[k],
            device_id={"node": other}, device_id_type=MESH,
        )

    def line(way, k, t):
        return pltpu.make_async_remote_copy(
            src_ref=sent.at[way, k, t], dst_ref=got.at[way, k, t],
            send_sem=line_send.at[way, k, t], recv_sem=line_recv.at[way, k, t],
            device_id={"node": (node + (2 if way == 0 else count - 2)) % count},
            device_id_type=MESH,
        )

    for d in range(1, experts):
        give(d).start()
    onward(0).start()
    xin[: slots, :] = xs[mine]

    weight = weight_at(0)
    for k in range(cuts):
        for j in range(3):
            cut_load(k, j).wait()

    @pl.loop(0, cuts)
    def _(k):
        @pl.loop(0, depth // tile_d)
        def _(i):
            at = pl.ds(pl.multiple_of(i * tile_d, tile_d), tile_d)
            par[k, at, :] = (zc[k, at, :].astype(f32) / weight).astype(bf16)

    def turned(tile):
        at = slice(tile * 128, (tile + 1) * 128)
        step = math.gcd(depth, 512)

        @pl.loop(0, 2 * depth // step)
        def _(i):
            cols = pl.ds(pl.multiple_of(i * step, step), step)
            xt[cols, at] = xin[at, cols].T

    def activations(pre, act, scale, hid_scale):
        gate = pre[:, :part] * scale
        upper = pre[:, part:] * scale
        act = act * hid_scale
        sig = jax.nn.sigmoid(gate)
        return (
            (act * upper * sig * (1.0 + gate * (1.0 - sig))).astype(bf16),
            (act * gate * sig).astype(bf16),
            (gate * sig * upper).astype(bf16),
        )

    def put(k, at, parts):
        for j in range(3):
            hid[k, at, j * part : (j + 1) * part] = parts[j]

    def forward(d, blocks):
        at = slice(d * slots, (d + blocks) * slots)

        @pl.loop(0, cuts)
        def _(k):
            pre = jnp.dot(xin[at, :depth], par[k, :, : 2 * part], preferred_element_type=f32)
            act = jnp.dot(xin[at, depth:], par[k, :, 2 * part :], preferred_element_type=f32)
            put(k, at, activations(pre, act, model_scale, hidden_scale))

    def gradients(k, at, size):
        down_at = pl.ds(pl.multiple_of(at + depth, size), size)
        at = pl.ds(pl.multiple_of(at, size), size)
        both = jnp.dot(xt[at, :], hid[k, :, : 2 * part], preferred_element_type=f32)
        down = jnp.dot(xt[down_at, :], hid[k, :, 2 * part :], preferred_element_type=f32)
        return jnp.concatenate([both * model_scale, down * hidden_scale], axis=1)

    forward(0, 1)
    done = 0
    for d in range(1, experts):
        give(d).wait_recv()
        onward(d).start()
        if d == experts - 2:
            forward(1, experts - 2)
        while (done + 1) * 128 <= (d + 1) * slots:
            turned(done)
            done = done + 1
    forward(experts - 1, 1)

    @pl.loop(0, cuts)
    def _(k):
        @pl.loop(0, depth // tile_d)
        def _(i):
            at = pl.ds(pl.multiple_of(i * tile_d, tile_d), tile_d)
            grads = gradients(k, i * tile_d, tile_d)
            zc[k, at, :] = (zc[k, at, :].astype(f32) - step_size * grads).astype(bf16)

    for d in range(experts):
        onward(d).wait_recv()

    @pl.loop(0, cuts)
    def _(k):
        pre = jnp.dot(xn[:, :depth], zc[k, :, : 2 * part], preferred_element_type=f32)
        act = jnp.dot(xn[:, depth:], zc[k, :, 2 * part :], preferred_element_type=f32)
        rs[k, :, : 2 * part] = pre.astype(bf16)
        rs[k, :, 2 * part :] = act.astype(bf16)
        result(k).start()

    def round_two(k):
        pre = jnp.dot(xin[:, :depth], zc[k, :, : 2 * part], preferred_element_type=f32)
        act = jnp.dot(xin[:, depth:], zc[k, :, 2 * part :], preferred_element_type=f32)
        result(k).wait_recv()
        pre = pre + rr[k, :, : 2 * part].astype(f32)
        act = act + rr[k, :, 2 * part :].astype(f32)
        parts = activations(
            pre, act, later[:, :1] * model_scale, later[:, :1] * hidden_scale
        )
        put(k, slice(0, total), parts)

        @pl.loop(0, chips)
        def _(i):
            at = pl.ds(pl.multiple_of(i * 2 * rows, 2 * rows), 2 * rows)
            grads = gradients(k, i * 2 * rows, 2 * rows)
            value = (keep * zc[k, at, :].astype(f32) - (step_size * factor) * grads).astype(bf16)
            second[k, i, 0] = value[:rows]
            second[k, i, 1] = value[rows:]

        pair(k).start()

    def term(k, t):
        return second[k, t, core].astype(f32) + came[k, t].astype(f32)

    def send_sums(k):
        pair(k).wait_recv()

        def rising(j, carry):
            t = chips - 1 - j
            sent[0, k, t] = term(k, t).astype(bf16)

            @pl.when(chip > 0)
            def _():
                line(0, k, t).wait_recv()
                sent[0, k, t] = (term(k, t) + got[0, k, t].astype(f32)).astype(bf16)

            line(0, k, t).start()
            return carry

        def falling(t, carry):
            sent[1, k, t] = term(k, t).astype(bf16)

            @pl.when(chip < chips - 1)
            def _():
                line(1, k, t).wait_recv()
                sent[1, k, t] = (term(k, t) + got[1, k, t].astype(f32)).astype(bf16)

            line(1, k, t).start()
            return carry

        @pl.when(chip * 2 < chips)
        def _():
            lax.fori_loop(0, chips - 1 - chip, rising, 0)
            lax.fori_loop(0, chip, falling, 0)

        @pl.when(chip * 2 >= chips)
        def _():
            lax.fori_loop(0, chip, falling, 0)
            lax.fori_loop(0, chips - 1 - chip, rising, 0)

    @pl.loop(0, cuts)
    def _(k):
        round_two(k)

        @pl.when(k > 0)
        def _():
            send_sums(k - 1)

    send_sums(cuts - 1)

    for k in range(cuts):
        value = term(k, chip)
        for j in range(3):
            out_ref[:, j * hidden + k * part : j * hidden + (k + 1) * part] = value[
                :, j * part : (j + 1) * part
            ]
        for way, there in ((0, chip > 0), (1, chip < chips - 1)):

            @pl.when(there)
            def _():
                line(way, k, chip).wait_recv()
                for j in range(3):
                    at = slice(j * hidden + k * part, j * hidden + (k + 1) * part)
                    cols = slice(j * part, (j + 1) * part)
                    out_ref[:, at] = out_ref[:, at] + got[way, k, chip, :, cols].astype(f32)

    for d in range(experts):
        if d > 0:
            give(d).wait_send()
        onward(d).wait_send()

    def drain(k, carry):
        result(k).wait_send()
        pair(k).wait_send()

        def up(t, c):
            line(0, k, t).wait_send()
            return c

        def down(t, c):
            line(1, k, t).wait_send()
            return c

        lax.fori_loop(chip + 1, chips, up, 0)
        lax.fori_loop(0, chip, down, 0)
        return carry

    lax.fori_loop(0, cuts, drain, 0)


def local(numerators, push_weights, tokens, cotangent, routing, gates):
    bf16, f32 = jnp.bfloat16, jnp.float32
    count, experts = lax.axis_size("node"), lax.axis_size("expert")
    depth, columns = numerators.shape[2:]
    own, top = routing.shape[1:]
    hidden = columns // 3
    part = math.gcd(hidden, 128)
    cuts = hidden // part
    width = 3 * part
    chips, rows = count // 2, depth // count
    slots = slots_of(own, top, experts)
    total = experts * slots
    vmem = pl.BlockSpec(memory_space=pltpu.VMEM)
    anywhere = pl.BlockSpec(memory_space=pl.ANY)
    dma = pltpu.SemaphoreType.DMA
    out = pl.pallas_call(
        functools.partial(steps_kernel, count, experts, cuts, slots),
        out_shape=jax.ShapeDtypeStruct((rows, columns), f32),
        in_specs=[pl.BlockSpec(memory_space=pltpu.SMEM)] + [anywhere] * 3 + [vmem] * 2,
        out_specs=vmem,
        scratch_shapes=[
            pltpu.VMEM((own, depth), bf16),
            pltpu.VMEM((own, depth), bf16),
            pltpu.VMEM((experts, slots, 2 * depth), bf16),
            pltpu.VMEM((total, 2 * depth), bf16),
            pltpu.VMEM((total, 2 * depth), bf16),
            pltpu.VMEM((2 * depth, total), bf16),
            pltpu.VMEM((cuts, depth, width), bf16),
            pltpu.VMEM((cuts, depth, width), bf16),
            pltpu.VMEM((cuts, total, width), bf16),
            pltpu.VMEM((cuts, total, width), bf16),
            pltpu.VMEM((cuts, total, width), bf16),
            pltpu.VMEM((cuts, chips, 2, rows, width), bf16),
            pltpu.VMEM((cuts, chips, rows, width), bf16),
            pltpu.VMEM((2, cuts, chips, rows, width), bf16),
            pltpu.VMEM((2, cuts, chips, rows, width), bf16),
            dma((2,)),
            dma((cuts, 3)),
            dma((experts,)),
            dma((experts,)),
            dma((experts,)),
            dma((experts,)),
            dma((cuts,)),
            dma((cuts,)),
            dma((cuts,)),
            dma((cuts,)),
            dma((2, cuts, chips)),
            dma((2, cuts, chips)),
        ],
        compiler_params=pltpu.CompilerParams(
            collective_id=0, has_side_effects=True, vmem_limit_bytes=60 * 1024 * 1024
        ),
    )(push_weights, numerators[0, 0], tokens[0], cotangent[0], routing[0], gates[0])
    return out[None]


def solution(mesh):
    placed = (
        P("node", "expert", None, None),
        P(),
        P("node", "expert", None),
        P("node", "expert", None),
        P("node", "expert", None),
        P("node", "expert", None),
    )
    return jax.shard_map(
        local, mesh=mesh, in_specs=placed, out_specs=P("expert", "node", None), check_vma=False
    )
```

```python
import functools
import math

import jax
import jax.numpy as jnp
from jax import lax
from jax.experimental import pallas as pl
from jax.experimental.pallas import tpu as pltpu
from jax.sharding import PartitionSpec as P

step_size = 1.0


HEAD = 16


def slots_of(tokens, top, experts):
    cap = 5 * tokens * top // (4 * experts) + 1
    return (cap // 8 * 8, 1) if cap % 8 == 1 else (-(-cap // 8) * 8, 0)


def steps_kernel(
    count, experts, cuts, slots, over,
    pw_hbm, z_hbm, x_hbm, g_hbm, routing_hbm, gates_hbm, out_ref,
    pw, routing, gates, xb, gb, xs, ext, ext_in, ext_n, xin, xn, xt, xnt, zc, par, hid, rs, rr, second, came, sent, got,
    load_sem, cut_sem, ext_send, ext_recv, ext_fwd, tok_send, tok_recv, fwd_send, fwd_recv, r_send, r_recv,
    pair_send, pair_recv, line_send, line_recv, turn,
):
    bf16, f32 = jnp.bfloat16, jnp.float32
    node, mine = lax.axis_index("node"), lax.axis_index("expert")
    chips = count // 2
    chip, core = node // 2, node % 2
    low = (chip * 2 < chips).astype(jnp.int32)
    inner = (chip > 0) & (chip < chips - 1)
    other = chip * 2 + (1 - core)
    before = (node + count - 1) % count
    depth, width = zc.shape[1:]
    part = width // 3
    hidden = part * cuts
    rows = depth // count
    own = x_hbm.shape[0]
    total = HEAD + experts * slots
    padded = xin.shape[0]
    folds = 2 * depth // 128
    model_scale = 1.0 / math.sqrt(depth)
    hidden_scale = 1.0 / math.sqrt(hidden)
    tile_d = math.gcd(depth, 256)
    MESH = pl.DeviceIdType.MESH

    loads = [
        pltpu.make_async_copy(x_hbm, xb, load_sem.at[0]),
        pltpu.make_async_copy(g_hbm, gb, load_sem.at[1]),
    ]
    small_loads = [
        pltpu.make_async_copy(routing_hbm, routing, load_sem.at[2]),
        pltpu.make_async_copy(gates_hbm, gates, load_sem.at[3]),
        pltpu.make_async_copy(pw_hbm, pw, load_sem.at[4]),
    ]
    for copy in small_loads:
        copy.start()
    for copy in loads:
        copy.start()

    def cut_load(k, j):
        return pltpu.make_async_copy(
            z_hbm.at[:, pl.ds(j * hidden + k * part, part)],
            zc.at[k, :, pl.ds(j * part, part)],
            cut_sem.at[k, j],
        )

    barrier = pltpu.get_barrier_semaphore()
    for d in range(1, experts):
        pl.semaphore_signal(
            barrier, inc=1, device_id={"expert": mine ^ d}, device_id_type=MESH
        )
    for by in (1, count - 1, 2, count - 2):
        pl.semaphore_signal(
            barrier, inc=1, device_id={"node": (node + by) % count}, device_id_type=MESH
        )

    for copy in small_loads:
        copy.wait()

    def weight_at(by):
        return pw[(node + by + count) % count]

    def last_at(by):
        total_w = weight_at(by) + weight_at(by - 1) + weight_at(by - 2) + weight_at(by - 3)
        return jnp.full((1, width), total_w * 0.25, f32)

    def factor_at(by):
        return (0.5 / last_at(by) + 0.5 / last_at(by + 2)) / count

    factor = factor_at(1)
    keep = 0.5 * (factor_at(0) + factor)
    later = 1.0 / jnp.full((1, width), weight_at(1) + weight_at(0), f32)

    names = lax.broadcasted_iota(jnp.int32, (16, own), 0)
    first, second_of = routing[0:1, :] == names, routing[1:2, :] == names
    chosen_t = jnp.where(first, 1.0, jnp.where(second_of, 1.0, 0.0))
    weighed_t = jnp.where(first, gates[0:1, :], jnp.where(second_of, gates[1:2, :], 0.0))
    ahead = jnp.where(
        lax.broadcasted_iota(jnp.int32, (own, own), 0)
        < lax.broadcasted_iota(jnp.int32, (own, own), 1),
        1.0, 0.0,
    ).astype(bf16)
    place = jnp.dot(chosen_t.astype(bf16), ahead, preferred_element_type=f32)
    place = jnp.where(chosen_t > 0.0, place, -1.0)
    slot = lax.broadcasted_iota(jnp.int32, (slots, own), 0).astype(f32)
    picks = [jnp.where(place == float(slots), 1.0, 0.0)] + [jnp.where(slot == place[e : e + 1, :], 1.0, 0.0) for e in range(experts)]
    pick = jnp.concatenate(picks, axis=0).astype(bf16)
    weighings = [weighed_t] + [weighed_t[e : e + 1, :] for e in range(experts)]
    row_gates = jnp.concatenate(
        [jnp.sum(p * v, axis=1, keepdims=True) for p, v in zip(picks, weighings)], axis=0
    )

    for copy in loads:
        copy.wait()
    for k in range(cuts):
        for j in range(3):
            cut_load(k, j).start()
    wide = math.gcd(depth, 256)
    for i in range(depth // wide):
        at = slice(i * wide, (i + 1) * wide)
        moved_x = jnp.dot(pick, xb[:, at], preferred_element_type=f32)
        moved_g = row_gates * jnp.dot(pick, gb[:, at], preferred_element_type=f32)
        for h, moved in enumerate((moved_x, moved_g)):
            start = h * depth + i * wide
            for e in range(experts):
                of = slice(HEAD + e * slots, HEAD + (e + 1) * slots)
                xs[e, :, start : start + wide] = moved[of].astype(bf16)
                for c in range(wide // 128 if over else 0):
                    row = start // 128 + c
                    ext[e, row : row + 1, :] = moved[e : e + 1, c * 128 : (c + 1) * 128]

    pl.semaphore_wait(barrier, experts - 1 + 4)

    def block(d):
        return pl.ds(d * slots + (HEAD if d > 0 else 0), slots)

    halves = [pl.ds(0, depth), pl.ds(depth, depth)]

    def give(d, h):
        return pltpu.make_async_remote_copy(
            src_ref=xs.at[mine ^ d, :, halves[h]], dst_ref=xin.at[block(d), halves[h]],
            send_sem=tok_send.at[d, h], recv_sem=tok_recv.at[d, h],
            device_id={"expert": mine ^ d}, device_id_type=MESH,
        )

    def onward(d, h):
        source = xs.at[mine, :, halves[h]] if d == 0 else xin.at[block(d), halves[h]]
        return pltpu.make_async_remote_copy(
            src_ref=source, dst_ref=xn.at[block(d), halves[h]],
            send_sem=fwd_send.at[d, h], recv_sem=fwd_recv.at[d, h],
            device_id={"node": before}, device_id_type=MESH,
        )

    def give_over(d):
        return pltpu.make_async_remote_copy(
            src_ref=ext.at[mine ^ d], dst_ref=ext_in.at[d],
            send_sem=ext_send.at[d], recv_sem=ext_recv.at[d],
            device_id={"expert": mine ^ d}, device_id_type=MESH,
        )

    def onward_over():
        return pltpu.make_async_remote_copy(
            src_ref=ext_in, dst_ref=ext_n, send_sem=ext_fwd.at[0], recv_sem=ext_fwd.at[1],
            device_id={"node": before}, device_id_type=MESH,
        )

    def unfold(source, target):
        lines = []
        for d in range(experts):
            value = source[d]
            lines.append(jnp.concatenate([value[c : c + 1] for c in range(folds)], axis=1))
        lines.append(jnp.zeros((HEAD - experts, 2 * depth), f32))
        target[slots : slots + HEAD, :] = jnp.concatenate(lines, axis=0).astype(bf16)

    def give_all():
        for d in range(1, experts if over else 0):
            give_over(d).start()
        for d in range(1, experts):
            for h in range(2):
                give(d, h).start()

    def arrive(d, h):
        give(d, h).wait_recv()
        onward(d, h).start()

    def result(k):
        return pltpu.make_async_remote_copy(
            src_ref=rs.at[k], dst_ref=rr.at[k],
            send_sem=r_send.at[k], recv_sem=r_recv.at[k],
            device_id={"node": before}, device_id_type=MESH,
        )

    def pair(k, t):
        return pltpu.make_async_remote_copy(
            src_ref=second.at[k, t, 1 - core], dst_ref=came.at[k, t],
            send_sem=pair_send.at[k, t], recv_sem=pair_recv.at[k, t],
            device_id={"node": other}, device_id_type=MESH,
        )

    def line(way, k, t):
        return pltpu.make_async_remote_copy(
            src_ref=sent.at[way, k, t], dst_ref=got.at[way, k, t],
            send_sem=line_send.at[way, k, t], recv_sem=line_recv.at[way, k, t],
            device_id={"node": (node + (2 if way == 0 else count - 2)) % count},
            device_id_type=MESH,
        )

    @pl.when(core == 0)
    def _():
        give_all()

    for h in range(2):
        onward(0, h).start()
    xin[:slots, :] = xs[mine]
    if over:
        ext_in[0] = ext[mine]
    else:
        xin[slots : slots + HEAD, :] = jnp.zeros((HEAD, 2 * depth), bf16)
        xn[slots : slots + HEAD, :] = jnp.zeros((HEAD, 2 * depth), bf16)
    if padded > total:
        xin[total:, :] = jnp.zeros((padded - total, 2 * depth), bf16)
        xn[total:, :] = jnp.zeros((padded - total, 2 * depth), bf16)
        for k in range(cuts):
            hid[k, total:, :] = jnp.zeros((padded - total, width), bf16)

    weight = weight_at(0)
    for k in range(cuts):
        for j in range(3):
            cut_load(k, j).wait()

    @pl.loop(0, cuts)
    def _(k):
        @pl.loop(0, depth // tile_d)
        def _(i):
            at = pl.ds(pl.multiple_of(i * tile_d, tile_d), tile_d)
            par[k, at, :] = (zc[k, at, :].astype(f32) / weight).astype(bf16)

    def turned(source, target, tile, part_of=(0, 2)):
        at = slice(tile * 128, (tile + 1) * 128)
        step = math.gcd(depth, 512)

        @pl.loop(part_of[0] * (depth // step), part_of[1] * (depth // step))
        def _(i):
            cols = pl.ds(pl.multiple_of(i * step, step), step)
            target[cols, at] = source[at, cols].T

    def next_head():
        if over:
            onward_over().wait_recv()
            unfold(ext_n, xn)

    def activations(pre, act, scale, hid_scale):
        gate = pre[:, :part] * scale
        upper = pre[:, part:] * scale
        act = act * hid_scale
        sig = jax.nn.sigmoid(gate)
        return (
            (act * upper * sig * (1.0 + gate * (1.0 - sig))).astype(bf16),
            (act * gate * sig).astype(bf16),
            (gate * sig * upper).astype(bf16),
        )

    def put(k, at, parts):
        for j in range(3):
            hid[k, at, j * part : (j + 1) * part] = parts[j]

    def forward_cut(k, at):
        pre = jnp.dot(xin[at, :depth], par[k, :, : 2 * part], preferred_element_type=f32)
        act = jnp.dot(xin[at, depth:], par[k, :, 2 * part :], preferred_element_type=f32)
        put(k, at, activations(pre, act, model_scale, hidden_scale))

    def forward(at):
        @pl.loop(0, cuts)
        def _(k):
            forward_cut(k, at)

    def gradients(xt, k, at, size):
        down_at = pl.ds(pl.multiple_of(at + depth, size), size)
        at = pl.ds(pl.multiple_of(at, size), size)
        both = jnp.dot(xt[at, :], hid[k, :, : 2 * part], preferred_element_type=f32)
        down = jnp.dot(xt[down_at, :], hid[k, :, 2 * part :], preferred_element_type=f32)
        return jnp.concatenate([both * model_scale, down * hidden_scale], axis=1)

    forward(slice(0, slots))

    @pl.when(core == 1)
    def _():
        pl.semaphore_wait(turn, 1)
        give_all()

    tiles = padded // 128
    last = experts - 1
    final = HEAD + last * slots
    early = final // 128

    if over:
        for d in range(1, experts):
            give_over(d).wait_recv()
        onward_over().start()
        unfold(ext_in, xin)

    for h in range(2):
        for d in range(1, last):
            arrive(d, h)
    for tile in range(early):
        turned(xin, xt, tile)
    forward(slice(slots, final))

    def next_tiles():
        next_head()
        for h in range(2):
            for d in range(last):
                onward(d, h).wait_recv()
        for tile in range(early):
            turned(xn, xnt, tile)
        for h in range(2):
            onward(last, h).wait_recv()
        for tile in range(early, tiles):
            turned(xn, xnt, tile)

    arrive(last, 0)
    for tile in range(early, tiles):
        turned(xin, xt, tile, (0, 1))

    @pl.when(core == 0)
    def _():
        for d in range(1, experts):
            for h in range(1 if d == last else 2):
                give(d, h).wait_send()
        pl.semaphore_signal(turn, inc=1, device_id={"node": other}, device_id_type=MESH)

    pl.when(core == 1)(next_tiles)

    arrive(last, 1)
    for tile in range(early, tiles):
        turned(xin, xt, tile, (1, 2))

    def round_one(k):
        forward_cut(k, slice(final, total))

        @pl.loop(0, depth // tile_d)
        def _(i):
            at = pl.ds(pl.multiple_of(i * tile_d, tile_d), tile_d)
            grads = gradients(xt, k, i * tile_d, tile_d)
            zc[k, at, :] = (zc[k, at, :].astype(f32) - step_size * grads).astype(bf16)

        pre = jnp.dot(xin[:total, :depth], zc[k, :, : 2 * part], preferred_element_type=f32)
        act = jnp.dot(xin[:total, depth:], zc[k, :, 2 * part :], preferred_element_type=f32)
        rs[k, :, : 2 * part] = pre.astype(bf16)
        rs[k, :, 2 * part :] = act.astype(bf16)
        result(k).start()

    def round_two(k):
        pre = jnp.dot(xn[:total, :depth], zc[k, :, : 2 * part], preferred_element_type=f32)
        act = jnp.dot(xn[:total, depth:], zc[k, :, 2 * part :], preferred_element_type=f32)
        result(k).wait_recv()
        pre = pre + rr[k, :, : 2 * part].astype(f32)
        act = act + rr[k, :, 2 * part :].astype(f32)
        parts = activations(
            pre, act, later[:, :1] * model_scale, later[:, :1] * hidden_scale
        )
        put(k, slice(0, total), parts)

        @pl.loop(0, chips)
        def _(i):
            t = i + low * (chips - 1 - 2 * i)
            at = pl.ds(pl.multiple_of(t * 2 * rows, 2 * rows), 2 * rows)
            grads = gradients(xnt, k, t * 2 * rows, 2 * rows)
            value = (keep * zc[k, at, :].astype(f32) - (step_size * factor) * grads).astype(bf16)
            second[k, t, 0] = value[:rows]
            second[k, t, 1] = value[rows:]
            pair(k, t).start()

    def term(k, t):
        return second[k, t, core].astype(f32) + came[k, t].astype(f32)

    def rising(k, j):
        t = chips - 1 - j
        pair(k, t).wait_recv()
        sent[0, k, t] = term(k, t).astype(bf16)

        @pl.when(chip > 0)
        def _():
            line(0, k, t).wait_recv()
            sent[0, k, t] = (term(k, t) + got[0, k, t].astype(f32)).astype(bf16)

        line(0, k, t).start()

    def falling(k, t):
        pair(k, t).wait_recv()
        sent[1, k, t] = term(k, t).astype(bf16)

        @pl.when(chip < chips - 1)
        def _():
            line(1, k, t).wait_recv()
            sent[1, k, t] = (term(k, t) + got[1, k, t].astype(f32)).astype(bf16)

        line(1, k, t).start()

    def send_sums(k):
        up = chips - 1 - chip - (chip == 0).astype(jnp.int32)
        down = chip - (chip == chips - 1).astype(jnp.int32)

        def rise(j, carry):
            rising(k, j)
            return carry

        def fall(t, carry):
            falling(k, t)
            return carry

        @pl.when(chip * 2 < chips)
        def _():
            lax.fori_loop(0, up, rise, 0)
            lax.fori_loop(0, down, fall, 0)

        @pl.when(chip * 2 >= chips)
        def _():
            lax.fori_loop(0, down, fall, 0)
            lax.fori_loop(0, up, rise, 0)

    def finish(k):
        pair(k, chip).wait_recv()
        value = term(k, chip)
        for j in range(3):
            out_ref[:, j * hidden + k * part : j * hidden + (k + 1) * part] = value[
                :, j * part : (j + 1) * part
            ]
        for way, there in ((0, chip > 0), (1, chip < chips - 1)):

            @pl.when(there)
            def _():
                line(way, k, chip).wait_recv()
                for j in range(3):
                    at = slice(j * hidden + k * part, j * hidden + (k + 1) * part)
                    cols = slice(j * part, (j + 1) * part)
                    out_ref[:, at] = out_ref[:, at] + got[way, k, chip, :, cols].astype(f32)

    @pl.when(core == 0)
    def _():
        pl.loop(0, cuts)(round_one)
        next_tiles()

    @pl.when(core == 1)
    def _():
        round_one(0)

    @pl.loop(0, cuts)
    def _(k):
        round_two(k)

        @pl.when(inner & (k > 0))
        def _():
            send_sums(k - 1)

        @pl.when(jnp.logical_not(inner))
        def _():
            send_sums(k)

        @pl.when((core == 1) & (k < cuts - 1))
        def _():
            round_one(k + 1)

    @pl.when(inner)
    def _():
        send_sums(cuts - 1)

    def nearest(k, carry):
        @pl.when(chip == 0)
        def _():
            rising(k, chips - 2)

        @pl.when(chip == chips - 1)
        def _():
            falling(k, chips - 2)

        return carry

    lax.fori_loop(0, cuts, nearest, 0)

    for k in range(cuts):
        finish(k)

    @pl.when(core == 1)
    def _():
        for d in range(1, experts):
            for h in range(2):
                give(d, h).wait_send()

    @pl.when(core == 0)
    def _():
        give(last, 1).wait_send()

    if over:
        onward_over().wait_send()
        for d in range(1, experts):
            give_over(d).wait_send()

    for d in range(experts):
        for h in range(2):
            onward(d, h).wait_send()

    def drain(k, carry):
        result(k).wait_send()

        def both(t, c):
            pair(k, t).wait_send()
            return c

        lax.fori_loop(0, chips, both, 0)

        def up(t, c):
            line(0, k, t).wait_send()
            return c

        def down(t, c):
            line(1, k, t).wait_send()
            return c

        lax.fori_loop(chip + 1, chips, up, 0)
        lax.fori_loop(0, chip, down, 0)
        return carry

    lax.fori_loop(0, cuts, drain, 0)


def local(numerators, push_weights, tokens, cotangent, routing, gates):
    bf16, f32 = jnp.bfloat16, jnp.float32
    count, experts = lax.axis_size("node"), lax.axis_size("expert")
    depth, columns = numerators.shape[2:]
    own, top = routing.shape[1:]
    hidden = columns // 3
    part = math.gcd(hidden, 128)
    cuts = hidden // part
    width = 3 * part
    chips, rows = count // 2, depth // count
    slots, over = slots_of(own, top, experts)
    total = HEAD + experts * slots
    folds = 2 * depth // 128
    padded = -(-total // 128) * 128
    vmem = pl.BlockSpec(memory_space=pltpu.VMEM)
    anywhere = pl.BlockSpec(memory_space=pltpu.HBM)
    dma = pltpu.SemaphoreType.DMA
    operands = [
        pltpu.with_memory_space_constraint(value, pltpu.HBM)
        for value in (
            push_weights, numerators[0, 0], tokens[0], cotangent[0], routing[0].T, gates[0].T
        )
    ]
    out = pl.pallas_call(
        functools.partial(steps_kernel, count, experts, cuts, slots, over),
        out_shape=jax.ShapeDtypeStruct((rows, columns), f32),
        in_specs=[anywhere] * 6,
        out_specs=vmem,
        scratch_shapes=[
            pltpu.SMEM((count,), f32),
            pltpu.VMEM((top, own), jnp.int32),
            pltpu.VMEM((top, own), f32),
            pltpu.VMEM((own, depth), bf16),
            pltpu.VMEM((own, depth), bf16),
            pltpu.VMEM((experts, slots, 2 * depth), bf16),
            pltpu.VMEM((experts, folds, 128), f32),
            pltpu.VMEM((experts, folds, 128), f32),
            pltpu.VMEM((experts, folds, 128), f32),
            pltpu.VMEM((padded, 2 * depth), bf16),
            pltpu.VMEM((padded, 2 * depth), bf16),
            pltpu.VMEM((2 * depth, padded), bf16),
            pltpu.VMEM((2 * depth, padded), bf16),
            pltpu.VMEM((cuts, depth, width), bf16),
            pltpu.VMEM((cuts, depth, width), bf16),
            pltpu.VMEM((cuts, padded, width), bf16),
            pltpu.VMEM((cuts, total, width), bf16),
            pltpu.VMEM((cuts, total, width), bf16),
            pltpu.VMEM((cuts, chips, 2, rows, width), bf16),
            pltpu.VMEM((cuts, chips, rows, width), bf16),
            pltpu.VMEM((2, cuts, chips, rows, width), bf16),
            pltpu.VMEM((2, cuts, chips, rows, width), bf16),
            dma((5,)),
            dma((cuts, 3)),
            dma((experts,)),
            dma((experts,)),
            dma((2,)),
            dma((experts, 2)),
            dma((experts, 2)),
            dma((experts, 2)),
            dma((experts, 2)),
            dma((cuts,)),
            dma((cuts,)),
            dma((cuts, chips)),
            dma((cuts, chips)),
            dma((2, cuts, chips)),
            dma((2, cuts, chips)),
            pltpu.SemaphoreType.REGULAR,
        ],
        compiler_params=pltpu.CompilerParams(
            collective_id=0, has_side_effects=True, vmem_limit_bytes=52 * 1024 * 1024
        ),
    )(*operands)
    return out[None]


def solution(mesh):
    placed = (
        P("node", "expert", None, None),
        P(),
        P("node", "expert", None),
        P("node", "expert", None),
        P("node", "expert", None),
        P("node", "expert", None),
    )
    return jax.shard_map(
        local, mesh=mesh, in_specs=placed, out_specs=P("expert", "node", None), check_vma=False
    )
```

```python
import functools
import math

import jax
import jax.numpy as jnp
from jax import lax
from jax.experimental import pallas as pl
from jax.experimental.pallas import tpu as pltpu
from jax.sharding import PartitionSpec as P

step_size = 1.0


HEAD = 16


def slots_of(tokens, top, experts):
    cap = 5 * tokens * top // (4 * experts) + 1
    return (cap // 8 * 8, 1) if cap % 8 == 1 else (-(-cap // 8) * 8, 0)


def steps_kernel(
    count, experts, cuts, slots, over,
    pw_hbm, z_hbm, x_hbm, g_hbm, routing_hbm, gates_hbm, out_ref,
    pw, routing, gates, xb, gb, xs, lines, ext, ext_in, ext_n, xin, xn, xt, xnt, zc, par, hid, rs, rr, second, came, sent, got,
    load_sem, cut_sem, ext_send, ext_recv, ext_fwd, tok_send, tok_recv, fwd_send, fwd_recv, r_send, r_recv,
    pair_send, pair_recv, line_send, line_recv, turn,
):
    bf16, f32 = jnp.bfloat16, jnp.float32
    node, mine = lax.axis_index("node"), lax.axis_index("expert")
    chips = count // 2
    chip, core = node // 2, node % 2
    low = (chip * 2 < chips).astype(jnp.int32)
    inner = (chip > 0) & (chip < chips - 1)
    other = chip * 2 + (1 - core)
    before = (node + count - 1) % count
    depth, width = zc.shape[1:]
    part = width // 3
    hidden = part * cuts
    rows = depth // count
    own = x_hbm.shape[0]
    total = HEAD + experts * slots
    padded = xin.shape[0]
    folds = 2 * depth // 128
    model_scale = 1.0 / math.sqrt(depth)
    hidden_scale = 1.0 / math.sqrt(hidden)
    tile_d = math.gcd(depth, 256)
    MESH = pl.DeviceIdType.MESH

    loads = [
        pltpu.make_async_copy(x_hbm, xb, load_sem.at[0]),
        pltpu.make_async_copy(g_hbm, gb, load_sem.at[1]),
    ]
    small_loads = [
        pltpu.make_async_copy(routing_hbm, routing, load_sem.at[2]),
        pltpu.make_async_copy(gates_hbm, gates, load_sem.at[3]),
        pltpu.make_async_copy(pw_hbm, pw, load_sem.at[4]),
    ]
    for copy in small_loads:
        copy.start()
    for copy in loads:
        copy.start()

    def cut_load(k, j):
        return pltpu.make_async_copy(
            z_hbm.at[:, pl.ds(j * hidden + k * part, part)],
            zc.at[k, :, pl.ds(j * part, part)],
            cut_sem.at[k, j],
        )

    barrier = pltpu.get_barrier_semaphore()
    for d in range(1, experts):
        pl.semaphore_signal(
            barrier, inc=1, device_id={"expert": mine ^ d}, device_id_type=MESH
        )
    for by in (1, count - 1, 2, count - 2):
        pl.semaphore_signal(
            barrier, inc=1, device_id={"node": (node + by) % count}, device_id_type=MESH
        )

    for copy in small_loads:
        copy.wait()

    def weight_at(by):
        return pw[(node + by + count) % count]

    def last_at(by):
        total_w = weight_at(by) + weight_at(by - 1) + weight_at(by - 2) + weight_at(by - 3)
        return jnp.full((1, width), total_w * 0.25, f32)

    def factor_at(by):
        return (0.5 / last_at(by) + 0.5 / last_at(by + 2)) / count

    factor = factor_at(1)
    keep = 0.5 * (factor_at(0) + factor)
    later = 1.0 / jnp.full((1, width), weight_at(1) + weight_at(0), f32)

    names = lax.broadcasted_iota(jnp.int32, (16, own), 0)
    first, second_of = routing[0:1, :] == names, routing[1:2, :] == names
    chosen_t = jnp.where(first, 1.0, jnp.where(second_of, 1.0, 0.0))
    weighed_t = jnp.where(first, gates[0:1, :], jnp.where(second_of, gates[1:2, :], 0.0))
    ahead = jnp.where(
        lax.broadcasted_iota(jnp.int32, (own, own), 0)
        < lax.broadcasted_iota(jnp.int32, (own, own), 1),
        1.0, 0.0,
    ).astype(bf16)
    place = jnp.dot(chosen_t.astype(bf16), ahead, preferred_element_type=f32)
    place = jnp.where(chosen_t > 0.0, place, -1.0)
    slot = lax.broadcasted_iota(jnp.int32, (slots, own), 0).astype(f32)
    picks = [jnp.where(place == float(slots), 1.0, 0.0)] + [jnp.where(slot == place[e : e + 1, :], 1.0, 0.0) for e in range(experts)]
    pick = jnp.concatenate(picks, axis=0).astype(bf16)
    weighings = [weighed_t] + [weighed_t[e : e + 1, :] for e in range(experts)]
    row_gates = jnp.concatenate(
        [jnp.sum(p * v, axis=1, keepdims=True) for p, v in zip(picks, weighings)], axis=0
    )

    for copy in loads:
        copy.wait()
    for k in range(cuts):
        for j in range(3):
            cut_load(k, j).start()
    wide = math.gcd(depth, 256)
    for i in range(depth // wide):
        at = slice(i * wide, (i + 1) * wide)
        moved_x = jnp.dot(pick, xb[:, at], preferred_element_type=f32)
        moved_g = row_gates * jnp.dot(pick, gb[:, at], preferred_element_type=f32)
        for h, moved in enumerate((moved_x, moved_g)):
            start = h * depth + i * wide
            for e in range(experts):
                of = slice(HEAD + e * slots, HEAD + (e + 1) * slots)
                xs[e, :, start : start + wide] = moved[of].astype(bf16)
                for c in range(wide // 128 if over else 0):
                    row = start // 128 + c
                    lines[e, row : row + 1, :] = moved[e : e + 1, c * 128 : (c + 1) * 128]
    if over:
        ext[...] = lines[...].astype(bf16)

    pl.semaphore_wait(barrier, experts - 1 + 4)

    def block(d):
        return pl.ds(d * slots + (HEAD if d > 0 else 0), slots)

    halves = [pl.ds(0, depth), pl.ds(depth, depth)]

    def give(d, h):
        return pltpu.make_async_remote_copy(
            src_ref=xs.at[mine ^ d, :, halves[h]], dst_ref=xin.at[block(d), halves[h]],
            send_sem=tok_send.at[d, h], recv_sem=tok_recv.at[d, h],
            device_id={"expert": mine ^ d}, device_id_type=MESH,
        )

    def onward(d, h):
        source = xs.at[mine, :, halves[h]] if d == 0 else xin.at[block(d), halves[h]]
        return pltpu.make_async_remote_copy(
            src_ref=source, dst_ref=xn.at[block(d), halves[h]],
            send_sem=fwd_send.at[d, h], recv_sem=fwd_recv.at[d, h],
            device_id={"node": before}, device_id_type=MESH,
        )

    def give_over(d):
        return pltpu.make_async_remote_copy(
            src_ref=ext.at[mine ^ d], dst_ref=ext_in.at[d],
            send_sem=ext_send.at[d], recv_sem=ext_recv.at[d],
            device_id={"expert": mine ^ d}, device_id_type=MESH,
        )

    def onward_over():
        return pltpu.make_async_remote_copy(
            src_ref=ext_in, dst_ref=ext_n, send_sem=ext_fwd.at[0], recv_sem=ext_fwd.at[1],
            device_id={"node": before}, device_id_type=MESH,
        )

    def unfold(source, target):
        whole = []
        for d in range(experts):
            value = source[d].astype(f32)
            whole.append(jnp.concatenate([value[c : c + 1] for c in range(folds)], axis=1))
        whole.append(jnp.zeros((HEAD - experts, 2 * depth), f32))
        target[slots : slots + HEAD, :] = jnp.concatenate(whole, axis=0).astype(bf16)

    def give_all():
        for d in range(1, experts if over else 0):
            give_over(d).start()
        for d in range(1, experts):
            for h in range(2):
                give(d, h).start()

    def arrive(d, h):
        give(d, h).wait_recv()
        onward(d, h).start()

    def result(k):
        return pltpu.make_async_remote_copy(
            src_ref=rs.at[k], dst_ref=rr.at[k],
            send_sem=r_send.at[k], recv_sem=r_recv.at[k],
            device_id={"node": before}, device_id_type=MESH,
        )

    def pair(k, t):
        return pltpu.make_async_remote_copy(
            src_ref=second.at[k, t, 1 - core], dst_ref=came.at[k, t],
            send_sem=pair_send.at[k, t], recv_sem=pair_recv.at[k, t],
            device_id={"node": other}, device_id_type=MESH,
        )

    def line(way, k, t):
        return pltpu.make_async_remote_copy(
            src_ref=sent.at[way, k, t], dst_ref=got.at[way, k, t],
            send_sem=line_send.at[way, k, t], recv_sem=line_recv.at[way, k, t],
            device_id={"node": (node + (2 if way == 0 else count - 2)) % count},
            device_id_type=MESH,
        )

    @pl.when(core == 0)
    def _():
        give_all()

    for h in range(2):
        onward(0, h).start()
    xin[:slots, :] = xs[mine]
    if over:
        ext_in[0] = ext[mine]
    else:
        xin[slots : slots + HEAD, :] = jnp.zeros((HEAD, 2 * depth), bf16)
        xn[slots : slots + HEAD, :] = jnp.zeros((HEAD, 2 * depth), bf16)
    if padded > total:
        xin[total:, :] = jnp.zeros((padded - total, 2 * depth), bf16)
        xn[total:, :] = jnp.zeros((padded - total, 2 * depth), bf16)
        for k in range(cuts):
            hid[k, total:, :] = jnp.zeros((padded - total, width), bf16)

    weight = weight_at(0)
    for k in range(cuts):
        for j in range(3):
            cut_load(k, j).wait()

    @pl.loop(0, cuts)
    def _(k):
        @pl.loop(0, depth // tile_d)
        def _(i):
            at = pl.ds(pl.multiple_of(i * tile_d, tile_d), tile_d)
            par[k, at, :] = (zc[k, at, :].astype(f32) / weight).astype(bf16)

    def turned(source, target, tile, part_of=(0, 2)):
        at = slice(tile * 128, (tile + 1) * 128)
        step = math.gcd(depth, 512)

        @pl.loop(part_of[0] * (depth // step), part_of[1] * (depth // step))
        def _(i):
            cols = pl.ds(pl.multiple_of(i * step, step), step)
            target[cols, at] = source[at, cols].T

    def next_head():
        if over:
            onward_over().wait_recv()
            unfold(ext_n, xn)

    def activations(pre, act, scale, hid_scale):
        gate = pre[:, :part] * scale
        upper = pre[:, part:] * scale
        act = act * hid_scale
        sig = jax.nn.sigmoid(gate)
        return (
            (act * upper * sig * (1.0 + gate * (1.0 - sig))).astype(bf16),
            (act * gate * sig).astype(bf16),
            (gate * sig * upper).astype(bf16),
        )

    def put(k, at, parts):
        for j in range(3):
            hid[k, at, j * part : (j + 1) * part] = parts[j]

    def forward_cut(k, at):
        pre = jnp.dot(xin[at, :depth], par[k, :, : 2 * part], preferred_element_type=f32)
        act = jnp.dot(xin[at, depth:], par[k, :, 2 * part :], preferred_element_type=f32)
        put(k, at, activations(pre, act, model_scale, hidden_scale))

    def forward(at):
        @pl.loop(0, cuts)
        def _(k):
            forward_cut(k, at)

    def gradients(xt, k, at, size):
        down_at = pl.ds(pl.multiple_of(at + depth, size), size)
        at = pl.ds(pl.multiple_of(at, size), size)
        both = jnp.dot(xt[at, :], hid[k, :, : 2 * part], preferred_element_type=f32)
        down = jnp.dot(xt[down_at, :], hid[k, :, 2 * part :], preferred_element_type=f32)
        return jnp.concatenate([both * model_scale, down * hidden_scale], axis=1)

    forward(slice(0, slots))

    @pl.when(core == 1)
    def _():
        pl.semaphore_wait(turn, 1)
        give_all()

    tiles = padded // 128
    last = experts - 1
    final = HEAD + last * slots
    early = final // 128

    if over:
        for d in range(1, experts):
            give_over(d).wait_recv()
        onward_over().start()
        unfold(ext_in, xin)

    for h in range(2):
        for d in range(1, last):
            arrive(d, h)
    for tile in range(early):
        turned(xin, xt, tile)
    forward(slice(slots, final))

    def next_tiles():
        next_head()
        for h in range(2):
            for d in range(last):
                onward(d, h).wait_recv()
        for tile in range(early):
            turned(xn, xnt, tile)
        for h in range(2):
            onward(last, h).wait_recv()
        for tile in range(early, tiles):
            turned(xn, xnt, tile)

    arrive(last, 0)
    for tile in range(early, tiles):
        turned(xin, xt, tile, (0, 1))

    @pl.when(core == 0)
    def _():
        for d in range(1, experts):
            for h in range(1 if d == last else 2):
                give(d, h).wait_send()
        pl.semaphore_signal(turn, inc=1, device_id={"node": other}, device_id_type=MESH)

    pl.when(core == 1)(next_tiles)

    arrive(last, 1)
    for tile in range(early, tiles):
        turned(xin, xt, tile, (1, 2))

    def round_one(k):
        forward_cut(k, slice(final, total))

        grads = gradients(xt, k, 0, depth)
        zc[k] = (zc[k].astype(f32) - step_size * grads).astype(bf16)

        pre = jnp.dot(xin[:total, :depth], zc[k, :, : 2 * part], preferred_element_type=f32)
        act = jnp.dot(xin[:total, depth:], zc[k, :, 2 * part :], preferred_element_type=f32)
        rs[k, :, : 2 * part] = pre.astype(bf16)
        rs[k, :, 2 * part :] = act.astype(bf16)
        result(k).start()

    def round_two(k):
        pre = jnp.dot(xn[:total, :depth], zc[k, :, : 2 * part], preferred_element_type=f32)
        act = jnp.dot(xn[:total, depth:], zc[k, :, 2 * part :], preferred_element_type=f32)
        result(k).wait_recv()
        pre = pre + rr[k, :, : 2 * part].astype(f32)
        act = act + rr[k, :, 2 * part :].astype(f32)
        parts = activations(
            pre, act, later[:, :1] * model_scale, later[:, :1] * hidden_scale
        )
        put(k, slice(0, total), parts)

        @pl.loop(0, chips, unroll=2)
        def _(i):
            t = i + low * (chips - 1 - 2 * i)
            at = pl.ds(pl.multiple_of(t * 2 * rows, 2 * rows), 2 * rows)
            grads = gradients(xnt, k, t * 2 * rows, 2 * rows)
            value = (keep * zc[k, at, :].astype(f32) - (step_size * factor) * grads).astype(bf16)
            second[k, t, 0] = value[:rows]
            second[k, t, 1] = value[rows:]
            pair(k, t).start()

    def term(k, t):
        return second[k, t, core].astype(f32) + came[k, t].astype(f32)

    def rising(k, j):
        t = chips - 1 - j
        pair(k, t).wait_recv()
        sent[0, k, t] = term(k, t).astype(bf16)

        @pl.when(chip > 0)
        def _():
            line(0, k, t).wait_recv()
            sent[0, k, t] = (term(k, t) + got[0, k, t].astype(f32)).astype(bf16)

        line(0, k, t).start()

    def falling(k, t):
        pair(k, t).wait_recv()
        sent[1, k, t] = term(k, t).astype(bf16)

        @pl.when(chip < chips - 1)
        def _():
            line(1, k, t).wait_recv()
            sent[1, k, t] = (term(k, t) + got[1, k, t].astype(f32)).astype(bf16)

        line(1, k, t).start()

    def rise_all(k):
        def rise(j, carry):
            rising(k, j)
            return carry

        lax.fori_loop(0, chips - 1 - chip - (chip == 0).astype(jnp.int32), rise, 0)

    def fall_all(k):
        def fall(t, carry):
            falling(k, t)
            return carry

        lax.fori_loop(0, chip - (chip == chips - 1).astype(jnp.int32), fall, 0)

    def long_way(k):
        pl.when(low == 1)(functools.partial(rise_all, k))
        pl.when(low == 0)(functools.partial(fall_all, k))

    def short_way(k):
        pl.when(low == 1)(functools.partial(fall_all, k))
        pl.when(low == 0)(functools.partial(rise_all, k))

    def finish(k):
        pair(k, chip).wait_recv()
        value = term(k, chip)
        for j in range(3):
            out_ref[:, j * hidden + k * part : j * hidden + (k + 1) * part] = value[
                :, j * part : (j + 1) * part
            ]
        for way, there in ((0, chip > 0), (1, chip < chips - 1)):

            @pl.when(there)
            def _():
                line(way, k, chip).wait_recv()
                for j in range(3):
                    at = slice(j * hidden + k * part, j * hidden + (k + 1) * part)
                    cols = slice(j * part, (j + 1) * part)
                    out_ref[:, at] = out_ref[:, at] + got[way, k, chip, :, cols].astype(f32)

    @pl.when(core == 0)
    def _():
        pl.loop(0, cuts)(round_one)
        next_tiles()

    @pl.when(core == 1)
    def _():
        round_one(0)

    @pl.loop(0, cuts)
    def _(k):
        round_two(k)

        ready = k - inner.astype(jnp.int32)

        @pl.when(ready >= 0)
        def _():
            long_way(ready)

        @pl.when((core == 1) & (k < cuts - 1))
        def _():
            round_one(k + 1)

        behind = k - 2 * inner.astype(jnp.int32)

        @pl.when(behind >= 0)
        def _():
            short_way(behind)

    @pl.when(inner)
    def _():
        long_way(cuts - 1)
        for k in range(max(cuts - 2, 0), cuts):
            short_way(k)

    def nearest(k, carry):
        @pl.when(chip == 0)
        def _():
            rising(k, chips - 2)

        @pl.when(chip == chips - 1)
        def _():
            falling(k, chips - 2)

        return carry

    lax.fori_loop(0, cuts, nearest, 0)

    for k in range(cuts):
        finish(k)

    @pl.when(core == 1)
    def _():
        for d in range(1, experts):
            for h in range(2):
                give(d, h).wait_send()

    @pl.when(core == 0)
    def _():
        give(last, 1).wait_send()

    if over:
        onward_over().wait_send()
        for d in range(1, experts):
            give_over(d).wait_send()

    for d in range(experts):
        for h in range(2):
            onward(d, h).wait_send()

    def drain(k, carry):
        result(k).wait_send()

        def both(t, c):
            pair(k, t).wait_send()
            return c

        lax.fori_loop(0, chips, both, 0)

        def up(t, c):
            line(0, k, t).wait_send()
            return c

        def down(t, c):
            line(1, k, t).wait_send()
            return c

        lax.fori_loop(chip + 1, chips, up, 0)
        lax.fori_loop(0, chip, down, 0)
        return carry

    lax.fori_loop(0, cuts, drain, 0)


def local(numerators, push_weights, tokens, cotangent, routing, gates):
    bf16, f32 = jnp.bfloat16, jnp.float32
    count, experts = lax.axis_size("node"), lax.axis_size("expert")
    depth, columns = numerators.shape[2:]
    own, top = routing.shape[1:]
    hidden = columns // 3
    part = math.gcd(hidden, 128)
    cuts = hidden // part
    width = 3 * part
    chips, rows = count // 2, depth // count
    slots, over = slots_of(own, top, experts)
    total = HEAD + experts * slots
    folds = 2 * depth // 128
    padded = -(-total // 128) * 128
    vmem = pl.BlockSpec(memory_space=pltpu.VMEM)
    anywhere = pl.BlockSpec(memory_space=pltpu.HBM)
    dma = pltpu.SemaphoreType.DMA
    operands = [
        pltpu.with_memory_space_constraint(value, pltpu.HBM)
        for value in (
            push_weights, numerators[0, 0], tokens[0], cotangent[0], routing[0].T, gates[0].T
        )
    ]
    out = pl.pallas_call(
        functools.partial(steps_kernel, count, experts, cuts, slots, over),
        out_shape=jax.ShapeDtypeStruct((rows, columns), f32),
        in_specs=[anywhere] * 6,
        out_specs=vmem,
        scratch_shapes=[
            pltpu.SMEM((count,), f32),
            pltpu.VMEM((top, own), jnp.int32),
            pltpu.VMEM((top, own), f32),
            pltpu.VMEM((own, depth), bf16),
            pltpu.VMEM((own, depth), bf16),
            pltpu.VMEM((experts, slots, 2 * depth), bf16),
            pltpu.VMEM((experts, folds, 128), f32),
            pltpu.VMEM((experts, folds, 128), bf16),
            pltpu.VMEM((experts, folds, 128), bf16),
            pltpu.VMEM((experts, folds, 128), bf16),
            pltpu.VMEM((padded, 2 * depth), bf16),
            pltpu.VMEM((padded, 2 * depth), bf16),
            pltpu.VMEM((2 * depth, padded), bf16),
            pltpu.VMEM((2 * depth, padded), bf16),
            pltpu.VMEM((cuts, depth, width), bf16),
            pltpu.VMEM((cuts, depth, width), bf16),
            pltpu.VMEM((cuts, padded, width), bf16),
            pltpu.VMEM((cuts, total, width), bf16),
            pltpu.VMEM((cuts, total, width), bf16),
            pltpu.VMEM((cuts, chips, 2, rows, width), bf16),
            pltpu.VMEM((cuts, chips, rows, width), bf16),
            pltpu.VMEM((2, cuts, chips, rows, width), bf16),
            pltpu.VMEM((2, cuts, chips, rows, width), bf16),
            dma((5,)),
            dma((cuts, 3)),
            dma((experts,)),
            dma((experts,)),
            dma((2,)),
            dma((experts, 2)),
            dma((experts, 2)),
            dma((experts, 2)),
            dma((experts, 2)),
            dma((cuts,)),
            dma((cuts,)),
            dma((cuts, chips)),
            dma((cuts, chips)),
            dma((2, cuts, chips)),
            dma((2, cuts, chips)),
            pltpu.SemaphoreType.REGULAR,
        ],
        compiler_params=pltpu.CompilerParams(
            collective_id=0, has_side_effects=True, vmem_limit_bytes=52 * 1024 * 1024
        ),
    )(*operands)
    return out[None]


def solution(mesh):
    placed = (
        P("node", "expert", None, None),
        P(),
        P("node", "expert", None),
        P("node", "expert", None),
        P("node", "expert", None),
        P("node", "expert", None),
    )
    return jax.shard_map(
        local, mesh=mesh, in_specs=placed, out_specs=P("expert", "node", None), check_vma=False
    )
```
